16 devices in a mesh: rep: 2 (over y, z), pp: 8 (over x, core).
Axes of the slice: x: 4, y: 2, z: 1, core: 2. Of those that a mesh axis runs over, the one named last changes fastest.
The devices are a block of a 4x4x8 slice.
Arguments:
- x: bfloat16 [32, 512, 512], P('rep'), parts along dimension 0
- dy: bfloat16 [32, 512, 512], P('rep'), parts along dimension 0
- w_gate: bfloat16 [8, 512, 1536], P('pp')
- w_up: bfloat16 [8, 512, 1536], P('pp')
- w_down: bfloat16 [8, 1536, 512], P('pp')
Outputs:
- output 1: bfloat16 [16, 512, 1536], P(('rep', 'pp')), parts along dimension 0
- output 2: bfloat16 [16, 512, 1536], P(('rep', 'pp')), parts along dimension 0
- output 3: bfloat16 [16, 1536, 512], P(('rep', 'pp')), parts along dimension 0
There are 2 independent parts. The reference program is written for one: setup_inputs(seed, part) draws one part's arguments, and reference() takes and returns one part's arrays. A program takes and returns all parts, laid end to end along the dimension named above; an argument that names none is the same for every part.
All inputs are finite; a program needn't handle non-finite values.
Results may differ from the reference program's by a relative error of at most 0.0238.
Values are sent between devices in bfloat16 or wider.
A program may use at most 768 MiB of HBM per device.

```python
import jax
import jax.numpy as jnp
from jax import lax

MICRO = 16
TOKENS = 512
D = 512
FF = 1536
LAYERS = 8
NAMES = ("w_gate", "w_up", "w_down")
SHAPES = {"w_gate": (LAYERS, D, FF), "w_up": (LAYERS, D, FF), "w_down": (LAYERS, FF, D)}


def bump(key, n, height):
    away = (jnp.arange(n, dtype=jnp.int32) - jax.random.randint(key, (), 0, n, jnp.int32)) % n
    return jnp.where(away < n // 8, height, 1.0)


def together(key, own, strength):
    shared = jax.random.normal(key, own.shape[1:], jnp.float32)
    return (own + strength * shared) * lax.rsqrt(1 + strength * strength)


def setup_inputs(seed: int = 0, part: int = 0) -> dict:
    kx, kdy, ka, kb, kz, kf, kh, kl, *kw = jax.random.split(jax.random.key(seed), 8 + len(NAMES))
    kx, kdy, ka, kb = (jax.random.fold_in(k, part) for k in (kx, kdy, ka, kb))
    shape = (MICRO, TOKENS, D)
    much_x, much_dy = jax.random.uniform(kz, (2,), jnp.float32, 0.0, 1.0)
    layers = 2.0 ** jax.random.uniform(kl, (LAYERS, 1, 1), jnp.float32, -1.0, 1.0)
    x = together(ka, jax.random.normal(kx, shape, jnp.float32), much_x) * bump(kf, D, 4.0)
    dy = together(kb, jax.random.normal(kdy, shape, jnp.float32), much_dy)
    drawn = {"x": x.astype(jnp.bfloat16), "dy": (dy * (MICRO * TOKENS) ** -0.5).astype(jnp.bfloat16)}
    for key, name in zip(kw, NAMES, strict=True):
        w = jax.random.normal(key, SHAPES[name], jnp.float32) * SHAPES[name][1] ** -0.5
        drawn[name] = (w * {"w_gate": 1.0, "w_up": bump(kh, FF, 4.0), "w_down": layers}[name]).astype(jnp.bfloat16)
    return drawn


def matmul(a, w):
    return jnp.dot(a, w, preferred_element_type=jnp.float32).astype(jnp.bfloat16)


def normed(h):
    wide = h.astype(jnp.float32)
    scale = lax.rsqrt(jnp.mean(wide**2, -1, keepdims=True) + 1e-6)
    return (wide * scale).astype(jnp.bfloat16)


def layer(h, w):
    a = normed(h)
    gate = jnp.dot(a, w["w_gate"], preferred_element_type=jnp.float32)
    up = jnp.dot(a, w["w_up"], preferred_element_type=jnp.float32)
    return h + matmul((jax.nn.silu(gate) * up).astype(jnp.bfloat16), w["w_down"])


def stack(weights, h):
    return lax.scan(lambda h, w: (layer(h, w), None), h, weights)[0]


def reference(x, dy, w_gate, w_up, w_down):
    weights = dict(zip(NAMES, (w_gate, w_up, w_down), strict=True))

    def take(so_far, one):
        h, by_y = one
        _, back = jax.vjp(lambda w: stack(w, h), weights)
        return jax.tree.map(lambda total, term: total + term.astype(jnp.float32), so_far, back(by_y)[0]), None

    none_yet = {name: jnp.zeros(w.shape, jnp.float32) for name, w in weights.items()}
    by_weights, _ = lax.scan(take, none_yet, (x, dy))
    return tuple(by_weights[name].astype(jnp.bfloat16) for name in NAMES)
```

```python
import functools

import jax
import jax.numpy as jnp
from jax import lax
from jax.experimental import pallas as pl
from jax.experimental.pallas import tpu as pltpu
from jax.sharding import PartitionSpec as P

F32, BF16 = jnp.float32, jnp.bfloat16
ROWS = 256
COLS = 256
SLOTS = 2
EPS = 1e-6


def lead(stages, me):
    table = [2, 3, 5, 6, 8, 9, 12, 13]
    ahead = 0
    for stage in range(stages):
        ahead = jnp.where(me == stage, table[min(stages - 1 - stage, len(table) - 1)], ahead)
    return ahead


def dot(a, b):
    return jnp.dot(a, b, preferred_element_type=F32)


def kernel(stages, x, dy, wg_in, wu_in, wd_in, og, ou, od, hp, hq, ha,
           wg, wu, wd, wgt, wut, wdt, acc_g, acc_u, acc_d, hs, ds, norm, turned, turned_dy,
           st_p, st_q, st_a, in_p, in_q, w_a, w_g, w_u, onward, back,
           sem_w, sem_h, sem_d, sem_f, sem_b, sem_st, sem_in, sem_act, sem_out):
    micro, tokens, d = x.shape
    ff = wg_in.shape[-1]
    chunks, tiles = tokens // ROWS, ff // COLS
    me = lax.axis_index("pp")
    first, last = me == 0, me == stages - 1
    inner = jnp.logical_not(last)
    later = jnp.logical_not(first)
    ahead = lead(stages, me)

    weights = [pltpu.make_async_copy(src.at[0], dst, sem_w.at[i]) for i, (src, dst) in enumerate(((wg_in, wg), (wu_in, wu), (wd_in, wd)))]
    for copy in weights:
        copy.start()

    def rows(c):
        return pl.ds(c * ROWS, ROWS)

    def load_x(i, c):
        return pltpu.make_async_copy(x.at[i, rows(c)], hs.at[i, rows(c)], sem_h.at[i, c])

    def load_dy(i, c):
        return pltpu.make_async_copy(dy.at[i, rows(c)], ds.at[i, rows(c)], sem_d.at[i, c])

    def send_h(i, c):
        slot = lax.rem(i, 2)
        return pltpu.make_async_remote_copy(onward.at[slot, c], hs.at[i, rows(c)], sem_f.at[slot, c], sem_h.at[i, c],
                                            device_id={"pp": me + 1}, device_id_type=pl.DeviceIdType.MESH)

    def send_d(i, c):
        return pltpu.make_async_remote_copy(back.at[c], ds.at[i, rows(c)], sem_b.at[c], sem_d.at[i, c],
                                            device_id={"pp": me - 1}, device_id_type=pl.DeviceIdType.MESH)

    def spill(i, c):
        return [pltpu.make_async_copy(src.at[c], dst.at[i, rows(c)], sem_st.at[k, c])
                for k, (src, dst) in enumerate(((st_p, hp), (st_q, hq), (st_a, ha)))]

    def fetch(i, c):
        return [pltpu.make_async_copy(src.at[i, rows(c)], dst.at[c], sem_in.at[k, c])
                for k, (src, dst) in enumerate(((hp, in_p), (hq, in_q)))]

    def fetch_act(i):
        slot = lax.rem(i, SLOTS)
        return pltpu.make_async_copy(ha.at[i], w_a.at[slot], sem_act.at[slot])

    @pl.when(first)
    def _():
        def body(i, _):
            for c in range(chunks):
                load_x(i, c).start()
            return 0
        lax.fori_loop(0, micro, body, 0)

    @pl.when(last)
    def _():
        def body(i, _):
            for c in range(chunks):
                load_dy(i, c).start()
            return 0
        lax.fori_loop(0, micro, body, 0)

    barrier = pltpu.get_barrier_semaphore()

    @pl.when(later)
    def _():
        pl.semaphore_signal(barrier, inc=1, device_id={"pp": me - 1}, device_id_type=pl.DeviceIdType.MESH)

    @pl.when(inner)
    def _():
        pl.semaphore_signal(barrier, inc=1, device_id={"pp": me + 1}, device_id_type=pl.DeviceIdType.MESH)

    for copy in weights:
        copy.wait()

    @pl.when(first | last)
    def _():
        pl.semaphore_wait(barrier, 1)

    @pl.when(later & inner)
    def _():
        pl.semaphore_wait(barrier, 2)

    def prepare():
        for n in range(tiles):
            cols = pl.ds(n * COLS, COLS)
            wgt[cols, :] = wg[:, cols].T
            wut[cols, :] = wu[:, cols].T
            wdt[:, cols] = wd[cols, :].T
            acc_g[:, cols] = jnp.zeros((d, COLS), F32)
            acc_u[:, cols] = jnp.zeros((d, COLS), F32)
            acc_d[:, cols] = jnp.zeros((d, COLS), F32)

    @pl.when(later)
    def _():
        prepare()

    def scale_of(wide):
        return lax.rsqrt(jnp.mean(wide * wide, -1, keepdims=True) + EPS)

    def forward(i, c):
        @pl.when(first)
        def _():
            load_x(i, c).wait()

        @pl.when(later)
        def _():
            send_h(i, c).wait_recv()

        wide = hs[i, rows(c), :].astype(F32)
        norm[...] = (wide * scale_of(wide)).astype(BF16)
        for n in range(tiles):
            cols = pl.ds(n * COLS, COLS)
            gate = dot(norm[...], wg[:, cols])
            up = dot(norm[...], wu[:, cols])
            sig = 1.0 / (1.0 + jnp.exp(-gate))
            silu = gate * sig
            st_p[c, :, cols] = silu
            st_q[c, :, cols] = up * (sig + silu * (1.0 - sig))
            st_a[c, :, cols] = (silu * up).astype(BF16)
        for copy in spill(i, c):
            copy.start()

        @pl.when(inner)
        def _():
            @pl.when(i > 1)
            def _():
                send_h(i - 2, c).wait_send()

            out = dot(st_a[c], wd[...]).astype(BF16)
            onward[lax.rem(i, 2), c] = (hs[i, rows(c), :].astype(F32) + out.astype(F32)).astype(BF16)
            send_h(i, c).start()

    def backward(i, c):
        slot = lax.rem(i, SLOTS)

        @pl.when(last)
        def _():
            load_dy(i, c).wait()

        @pl.when(inner)
        def _():
            send_d(i, c).wait_recv()

        for copy in fetch(i, c):
            copy.wait()
        for n in range(tiles):
            cols = pl.ds(n * COLS, COLS)
            by_act = dot(ds[i, rows(c), :], wdt[:, cols]).astype(BF16).astype(F32)
            w_g[slot, rows(c), cols] = (by_act * in_q[c, :, cols]).astype(BF16)
            w_u[slot, rows(c), cols] = (by_act * in_p[c, :, cols]).astype(BF16)

        @pl.when(later)
        def _():
            @pl.when(i > 0)
            def _():
                send_d(i - 1, c).wait_send()

            by_gate = dot(w_g[slot, rows(c), :], wgt[...]).astype(BF16)
            by_up = dot(w_u[slot, rows(c), :], wut[...]).astype(BF16)
            by_a = (by_gate.astype(F32) + by_up.astype(F32)).astype(BF16).astype(F32)
            wide = hs[i, rows(c), :].astype(F32)
            scale = scale_of(wide)
            along = jnp.mean(by_a * wide, -1, keepdims=True) * (scale * scale * scale)
            by_h = (by_a * scale - wide * along).astype(BF16)
            back[c] = (ds[i, rows(c), :].astype(F32) + by_h.astype(F32)).astype(BF16)
            send_d(i, c).start()

    def weight(i):
        slot = lax.rem(i, SLOTS)
        for c in range(chunks):
            wide = hs[i, rows(c), :].astype(F32)
            turned[:, rows(c)] = (wide * scale_of(wide)).astype(BF16).T
            turned_dy[:, rows(c)] = ds[i, rows(c), :].T
        fetch_act(i).wait()
        for n in range(tiles):
            cols = pl.ds(n * COLS, COLS)
            for acc, left, right in ((acc_g, turned, w_g), (acc_u, turned, w_u), (acc_d, turned_dy, w_a)):
                acc[:, cols] += dot(left[...], right[slot, :, cols]).astype(BF16).astype(F32)

    def step(t, _):
        @pl.when((t > 0) & (t <= micro))
        def _():
            for c in range(chunks):
                for copy in spill(t - 1, c):
                    copy.wait()

        @pl.when(t < micro)
        def _():
            for c in range(chunks):
                forward(t, c)

        @pl.when(first & (t == 0))
        def _():
            prepare()

        b = t - ahead

        @pl.when((b >= 0) & (b < micro))
        def _():
            fetch_act(b).start()
            for c in range(chunks):
                backward(b, c)

        @pl.when((b >= -1) & (b < micro - 1))
        def _():
            for c in range(chunks):
                for copy in fetch(b + 1, c):
                    copy.start()

        w = b - (SLOTS - 1)

        @pl.when((w >= 0) & (w < micro))
        def _():
            weight(w)
        return 0

    lax.fori_loop(0, micro + ahead + SLOTS - 1, step, 0)

    @pl.when(later)
    def _():
        for c in range(chunks):
            send_d(micro - 1, c).wait_send()

    @pl.when(inner)
    def _():
        for c in range(chunks):
            send_h(micro - 2, c).wait_send()
            send_h(micro - 1, c).wait_send()

    for n in range(tiles):
        cols = pl.ds(n * COLS, COLS)
        w_g[0, :, cols] = acc_g[:, cols].astype(BF16)
        w_u[0, :, cols] = acc_u[:, cols].astype(BF16)
        wd[cols, :] = acc_d[:, cols].astype(BF16).T
    results = [pltpu.make_async_copy(src, dst.at[0], sem_out.at[i]) for i, (src, dst) in enumerate(((w_g.at[0], og), (w_u.at[0], ou), (wd, od)))]
    for copy in results:
        copy.start()
    for copy in results:
        copy.wait()


def solution(mesh):
    stages = mesh.shape["pp"]

    def step(x, dy, w_gate, w_up, w_down):
        micro, tokens, d = x.shape
        ff = w_gate.shape[-1]
        chunks = tokens // ROWS
        hbm = pl.BlockSpec(memory_space=pl.ANY)
        vmem, dma = pltpu.VMEM, pltpu.SemaphoreType.DMA
        outs = pl.pallas_call(
            functools.partial(kernel, stages),
            out_shape=[
                jax.ShapeDtypeStruct(w_gate.shape, BF16),
                jax.ShapeDtypeStruct(w_up.shape, BF16),
                jax.ShapeDtypeStruct(w_down.shape, BF16),
                jax.ShapeDtypeStruct((micro, tokens, ff), F32),
                jax.ShapeDtypeStruct((micro, tokens, ff), F32),
                jax.ShapeDtypeStruct((micro, tokens, ff), BF16),
            ],
            in_specs=[hbm] * 5,
            out_specs=[hbm] * 6,
            scratch_shapes=[
                vmem((d, ff), BF16), vmem((d, ff), BF16), vmem((ff, d), BF16),
                vmem((ff, d), BF16), vmem((ff, d), BF16), vmem((d, ff), BF16),
                vmem((d, ff), F32), vmem((d, ff), F32), vmem((d, ff), F32),
                vmem((micro, tokens, d), BF16), vmem((micro, tokens, d), BF16),
                vmem((ROWS, d), BF16), vmem((d, tokens), BF16), vmem((d, tokens), BF16),
                vmem((chunks, ROWS, ff), F32), vmem((chunks, ROWS, ff), F32), vmem((chunks, ROWS, ff), BF16),
                vmem((chunks, ROWS, ff), F32), vmem((chunks, ROWS, ff), F32),
                vmem((SLOTS, tokens, ff), BF16), vmem((SLOTS, tokens, ff), BF16), vmem((SLOTS, tokens, ff), BF16),
                vmem((2, chunks, ROWS, d), BF16), vmem((chunks, ROWS, d), BF16),
                dma((3,)), dma((micro, chunks)), dma((micro, chunks)), dma((2, chunks)), dma((chunks,)),
                dma((3, chunks)), dma((2, chunks)), dma((SLOTS,)), dma((3,)),
            ],
            compiler_params=pltpu.CompilerParams(collective_id=0, has_side_effects=True, vmem_limit_bytes=67000000),
        )(x, dy, w_gate, w_up, w_down)
        return tuple(outs[:3])

    return jax.shard_map(
        step,
        mesh=mesh,
        in_specs=(P("rep", None, None),) * 2 + (P("pp", None, None),) * 3,
        out_specs=(P(("rep", "pp"), None, None),) * 3,
        check_vma=False,
    )
```

```python
import functools

import jax
import jax.numpy as jnp
from jax import lax
from jax.experimental import pallas as pl
from jax.experimental.pallas import tpu as pltpu
from jax.sharding import PartitionSpec as P

F32, BF16 = jnp.float32, jnp.bfloat16
ROWS = 256
COLS = 256
SLOTS = 2
EPS = 1e-6


def lead(stages, me):
    table = [2, 3, 5, 6, 8, 9, 12, 13]
    ahead = 0
    for stage in range(stages):
        ahead = jnp.where(me == stage, table[min(stages - 1 - stage, len(table) - 1)], ahead)
    return ahead


def dot(a, b):
    return jnp.dot(a, b, preferred_element_type=F32)


def kernel(stages, x, dy, wg_in, wu_in, wd_in, og, ou, od, hp, hq, ha,
           wg, wu, wd, wgt, wut, wdt, acc_g, acc_u, acc_d, hs, ds, norm, turned, turned_dy,
           st_p, st_q, st_a, in_p, in_q, w_a, w_g, w_u, onward, back,
           sem_w, sem_h, sem_d, sem_f, sem_b, sem_st, sem_in, sem_act, sem_out):
    micro, tokens, d = x.shape
    ff = wg_in.shape[-1]
    chunks, tiles = tokens // ROWS, ff // COLS
    me = lax.axis_index("pp")
    first, last = me == 0, me == stages - 1
    inner = jnp.logical_not(last)
    later = jnp.logical_not(first)
    ahead = lead(stages, me)

    weights = [pltpu.make_async_copy(src.at[0], dst, sem_w.at[i]) for i, (src, dst) in enumerate(((wg_in, wg), (wu_in, wu), (wd_in, wd)))]
    for copy in weights:
        copy.start()

    def rows(c):
        return pl.ds(c * ROWS, ROWS)

    def load_x(i, c):
        return pltpu.make_async_copy(x.at[i, rows(c)], hs.at[i, rows(c)], sem_h.at[i, c])

    def load_dy(i, c):
        return pltpu.make_async_copy(dy.at[i, rows(c)], ds.at[i, rows(c)], sem_d.at[i, c])

    def send_h(i, c):
        slot = lax.rem(i, 2)
        return pltpu.make_async_remote_copy(onward.at[slot, c], hs.at[i, rows(c)], sem_f.at[slot, c], sem_h.at[i, c],
                                            device_id={"pp": me + 1}, device_id_type=pl.DeviceIdType.MESH)

    def send_d(i, c):
        return pltpu.make_async_remote_copy(back.at[c], ds.at[i, rows(c)], sem_b.at[c], sem_d.at[i, c],
                                            device_id={"pp": me - 1}, device_id_type=pl.DeviceIdType.MESH)

    def spill(i, c):
        return [pltpu.make_async_copy(src.at[c], dst.at[i, rows(c)], sem_st.at[k, c])
                for k, (src, dst) in enumerate(((st_p, hp), (st_q, hq), (st_a, ha)))]

    def fetch(i, c):
        return [pltpu.make_async_copy(src.at[i, rows(c)], dst.at[c], sem_in.at[k, c])
                for k, (src, dst) in enumerate(((hp, in_p), (hq, in_q)))]

    def fetch_act(i):
        slot = lax.rem(i, SLOTS)
        return pltpu.make_async_copy(ha.at[i], w_a.at[slot], sem_act.at[slot])

    @pl.when(first)
    def _():
        def body(i, _):
            for c in range(chunks):
                load_x(i, c).start()
            return 0
        lax.fori_loop(0, micro, body, 0)

    @pl.when(last)
    def _():
        def body(i, _):
            for c in range(chunks):
                load_dy(i, c).start()
            return 0
        lax.fori_loop(0, micro, body, 0)

    barrier = pltpu.get_barrier_semaphore()

    @pl.when(later)
    def _():
        pl.semaphore_signal(barrier, inc=1, device_id={"pp": me - 1}, device_id_type=pl.DeviceIdType.MESH)

    @pl.when(inner)
    def _():
        pl.semaphore_signal(barrier, inc=1, device_id={"pp": me + 1}, device_id_type=pl.DeviceIdType.MESH)

    for copy in weights:
        copy.wait()

    @pl.when(first | last)
    def _():
        pl.semaphore_wait(barrier, 1)

    @pl.when(later & inner)
    def _():
        pl.semaphore_wait(barrier, 2)

    def prepare():
        for n in range(tiles):
            cols = pl.ds(n * COLS, COLS)
            wgt[cols, :] = wg[:, cols].T
            wut[cols, :] = wu[:, cols].T
            wdt[:, cols] = wd[cols, :].T
            acc_g[:, cols] = jnp.zeros((d, COLS), F32)
            acc_u[:, cols] = jnp.zeros((d, COLS), F32)
            acc_d[:, cols] = jnp.zeros((d, COLS), F32)

    @pl.when(later)
    def _():
        prepare()

    def scale_of(wide):
        return lax.rsqrt(jnp.mean(wide * wide, -1, keepdims=True) + EPS)

    def weight(i, n, acc, left, right):
        slot, cols = lax.rem(i, SLOTS), pl.ds(n * COLS, COLS)
        acc[:, cols] += dot(left[slot], right[slot, :, cols]).astype(BF16).astype(F32)

    def parts(tile_numbers):
        return [(n, *arrays) for n in tile_numbers for arrays in ((acc_g, turned, w_g), (acc_u, turned, w_u), (acc_d, turned_dy, w_a))]

    def forward(i, c, onwards, w):
        fill = [] if w is None else parts([c])
        wide = hs[i, rows(c), :].astype(F32)
        norm[...] = (wide * scale_of(wide)).astype(BF16)
        for part in fill[:2]:
            weight(w, *part)
        for n in range(tiles):
            cols = pl.ds(n * COLS, COLS)
            gate = dot(norm[...], wg[:, cols])
            up = dot(norm[...], wu[:, cols])
            sig = 1.0 / (1.0 + jnp.exp(-gate))
            silu = gate * sig
            st_p[c, :, cols] = silu
            st_q[c, :, cols] = up * (sig + silu * (1.0 - sig))
            st_a[c, :, cols] = (silu * up).astype(BF16)
        for part in fill[2:]:
            weight(w, *part)
        if onwards:
            out = dot(st_a[c], wd[...]).astype(BF16)
            onward[lax.rem(i, 2), c] = (hs[i, rows(c), :].astype(F32) + out.astype(F32)).astype(BF16)
            send_h(i, c).start()
        for copy in spill(i, c):
            copy.start()

    def backward(i, c, w):
        slot = lax.rem(i, SLOTS)
        each = (tiles - chunks) // chunks
        fill = [] if w is None else parts(range(chunks + c * each, chunks + (c + 1) * each))
        wide = hs[i, rows(c), :].astype(F32)
        scale = scale_of(wide)
        turned[slot, :, rows(c)] = (wide * scale).astype(BF16).T
        turned_dy[slot, :, rows(c)] = ds[i, rows(c), :].T
        for n in range(tiles):
            cols = pl.ds(n * COLS, COLS)
            by_act = dot(ds[i, rows(c), :], wdt[:, cols]).astype(BF16).astype(F32)
            w_g[slot, rows(c), cols] = (by_act * in_q[c, :, cols]).astype(BF16)
            w_u[slot, rows(c), cols] = (by_act * in_p[c, :, cols]).astype(BF16)
        for part in fill[:2]:
            weight(w, *part)
        by_gate = dot(w_g[slot, rows(c), :], wgt[...]).astype(BF16)
        by_up = dot(w_u[slot, rows(c), :], wut[...]).astype(BF16)
        by_a = (by_gate.astype(F32) + by_up.astype(F32)).astype(BF16).astype(F32)
        along = jnp.mean(by_a * wide, -1, keepdims=True) * (scale * scale * scale)
        by_h = (by_a * scale - wide * along).astype(BF16)
        back[c] = (ds[i, rows(c), :].astype(F32) + by_h.astype(F32)).astype(BF16)
        for part in fill[2:]:
            weight(w, *part)

    def step(t, _):
        b = t - ahead
        w = b - (SLOTS - 1)
        has_f, has_b, has_w = t < micro, (b >= 0) & (b < micro), (w >= 0) & (w < micro)

        @pl.when(has_w)
        def _():
            fetch_act(w).wait()

        @pl.when((t > 0) & (t <= micro))
        def _():
            for c in range(chunks):
                for copy in spill(t - 1, c):
                    copy.wait()

        @pl.when(has_b)
        def _():
            fetch_act(b).start()

        for c in range(chunks):
            @pl.when(has_f)
            def _():
                @pl.when(first)
                def _():
                    load_x(t, c).wait()

                @pl.when(later)
                def _():
                    send_h(t, c).wait_recv()

                @pl.when(inner & (t > 1))
                def _():
                    send_h(t - 2, c).wait_send()

            for onwards in (True, False):
                at = inner if onwards else last

                @pl.when(has_f & at & has_w)
                def _():
                    forward(t, c, onwards, w)

                @pl.when(has_f & at & jnp.logical_not(has_w))
                def _():
                    forward(t, c, onwards, None)

        @pl.when(first & (t == 0))
        def _():
            prepare()

        @pl.when(has_w & jnp.logical_not(has_f))
        def _():
            for part in parts(range(chunks)):
                weight(w, *part)

        for c in range(chunks):
            @pl.when(has_b)
            def _():
                @pl.when(last)
                def _():
                    load_dy(b, c).wait()

                @pl.when(inner)
                def _():
                    send_d(b, c).wait_recv()

                @pl.when(later & (b > 0))
                def _():
                    send_d(b - 1, c).wait_send()

                for copy in fetch(b, c):
                    copy.wait()

            @pl.when(has_b & has_w)
            def _():
                backward(b, c, w)

            @pl.when(has_b & jnp.logical_not(has_w))
            def _():
                backward(b, c, None)

            @pl.when(has_b & later)
            def _():
                send_d(b, c).start()

            @pl.when((b >= -1) & (b < micro - 1))
            def _():
                for copy in fetch(b + 1, c):
                    copy.start()

        @pl.when(has_w & jnp.logical_not(has_b))
        def _():
            for part in parts(range(chunks, tiles)):
                weight(w, *part)
        return 0

    lax.fori_loop(0, micro + ahead + SLOTS - 1, step, 0)

    @pl.when(later)
    def _():
        for c in range(chunks):
            send_d(micro - 1, c).wait_send()

    @pl.when(inner)
    def _():
        for c in range(chunks):
            send_h(micro - 2, c).wait_send()
            send_h(micro - 1, c).wait_send()

    for n in range(tiles):
        cols = pl.ds(n * COLS, COLS)
        w_g[0, :, cols] = acc_g[:, cols].astype(BF16)
        w_u[0, :, cols] = acc_u[:, cols].astype(BF16)
        wd[cols, :] = acc_d[:, cols].astype(BF16).T
    results = [pltpu.make_async_copy(src, dst.at[0], sem_out.at[i]) for i, (src, dst) in enumerate(((w_g.at[0], og), (w_u.at[0], ou), (wd, od)))]
    for copy in results:
        copy.start()
    for copy in results:
        copy.wait()


def solution(mesh):
    stages = mesh.shape["pp"]

    def step(x, dy, w_gate, w_up, w_down):
        micro, tokens, d = x.shape
        ff = w_gate.shape[-1]
        chunks = tokens // ROWS
        hbm = pl.BlockSpec(memory_space=pl.ANY)
        vmem, dma = pltpu.VMEM, pltpu.SemaphoreType.DMA
        outs = pl.pallas_call(
            functools.partial(kernel, stages),
            out_shape=[
                jax.ShapeDtypeStruct(w_gate.shape, BF16),
                jax.ShapeDtypeStruct(w_up.shape, BF16),
                jax.ShapeDtypeStruct(w_down.shape, BF16),
                jax.ShapeDtypeStruct((micro, tokens, ff), F32),
                jax.ShapeDtypeStruct((micro, tokens, ff), F32),
                jax.ShapeDtypeStruct((micro, tokens, ff), BF16),
            ],
            in_specs=[hbm] * 5,
            out_specs=[hbm] * 6,
            scratch_shapes=[
                vmem((d, ff), BF16), vmem((d, ff), BF16), vmem((ff, d), BF16),
                vmem((ff, d), BF16), vmem((ff, d), BF16), vmem((d, ff), BF16),
                vmem((d, ff), F32), vmem((d, ff), F32), vmem((d, ff), F32),
                vmem((micro, tokens, d), BF16), vmem((micro, tokens, d), BF16),
                vmem((ROWS, d), BF16), vmem((SLOTS, d, tokens), BF16), vmem((SLOTS, d, tokens), BF16),
                vmem((chunks, ROWS, ff), F32), vmem((chunks, ROWS, ff), F32), vmem((chunks, ROWS, ff), BF16),
                vmem((chunks, ROWS, ff), F32), vmem((chunks, ROWS, ff), F32),
                vmem((SLOTS, tokens, ff), BF16), vmem((SLOTS, tokens, ff), BF16), vmem((SLOTS, tokens, ff), BF16),
                vmem((2, chunks, ROWS, d), BF16), vmem((chunks, ROWS, d), BF16),
                dma((3,)), dma((micro, chunks)), dma((micro, chunks)), dma((2, chunks)), dma((chunks,)),
                dma((3, chunks)), dma((2, chunks)), dma((SLOTS,)), dma((3,)),
            ],
            compiler_params=pltpu.CompilerParams(collective_id=0, has_side_effects=True, vmem_limit_bytes=67000000),
        )(x, dy, w_gate, w_up, w_down)
        return tuple(outs[:3])

    return jax.shard_map(
        step,
        mesh=mesh,
        in_specs=(P("rep", None, None),) * 2 + (P("pp", None, None),) * 3,
        out_specs=(P(("rep", "pp"), None, None),) * 3,
        check_vma=False,
    )
```

```python
import functools

import jax
import jax.numpy as jnp
from jax import lax
from jax.experimental import pallas as pl
from jax.experimental.pallas import tpu as pltpu
from jax.sharding import PartitionSpec as P

F32, BF16 = jnp.float32, jnp.bfloat16
ROWS = 256
COLS = 256
SLOTS = 2
EPS = 1e-6


def lead(stages, me):
    table = [1, 2, 4, 5, 7, 8, 14, 16]
    ahead = 0
    for stage in range(stages):
        ahead = jnp.where(me == stage, table[min(stages - 1 - stage, len(table) - 1)], ahead)
    return ahead


def dot(a, b):
    return jnp.dot(a, b, preferred_element_type=F32)


def kernel(stages, x, dy, wg_in, wu_in, wd_in, og, ou, od, hp, hq, ha,
           wg, wu, wd, wgt, wut, wdt, acc_g, acc_u, acc_d, hs, ds, norm, turned, turned_dy,
           st_p, st_q, st_a, in_p, in_q, w_a, w_g, w_u, onward, back,
           sem_w, sem_h, sem_d, sem_f, sem_b, sem_st, sem_in, sem_act, sem_out):
    micro, tokens, d = x.shape
    ff = wg_in.shape[-1]
    chunks, tiles = tokens // ROWS, ff // COLS
    me = lax.axis_index("pp")
    first, last = me == 0, me == stages - 1
    inner = jnp.logical_not(last)
    later = jnp.logical_not(first)
    ahead = lead(stages, me)

    weights = [pltpu.make_async_copy(src.at[0], dst, sem_w.at[i]) for i, (src, dst) in enumerate(((wg_in, wg), (wu_in, wu), (wd_in, wd)))]

    def rows(c):
        return pl.ds(c * ROWS, ROWS)

    def load_x(i, c):
        return pltpu.make_async_copy(x.at[i, rows(c)], hs.at[i, rows(c)], sem_h.at[i, c])

    def load_dy(i, c):
        return pltpu.make_async_copy(dy.at[i, rows(c)], ds.at[i, rows(c)], sem_d.at[i, c])

    def send_h(i, c):
        slot = lax.rem(i, 2)
        return pltpu.make_async_remote_copy(onward.at[slot, c], hs.at[i, rows(c)], sem_f.at[slot, c], sem_h.at[i, c],
                                            device_id={"pp": me + 1}, device_id_type=pl.DeviceIdType.MESH)

    def send_d(i, c):
        return pltpu.make_async_remote_copy(back.at[c], ds.at[i, rows(c)], sem_b.at[c], sem_d.at[i, c],
                                            device_id={"pp": me - 1}, device_id_type=pl.DeviceIdType.MESH)

    def spill(i, c):
        return [pltpu.make_async_copy(src.at[c], dst.at[i, rows(c)], sem_st.at[k, c])
                for k, (src, dst) in enumerate(((st_p, hp), (st_q, hq), (st_a, ha)))]

    def fetch(i, c):
        return [pltpu.make_async_copy(src.at[i, rows(c)], dst.at[c], sem_in.at[k, c])
                for k, (src, dst) in enumerate(((hp, in_p), (hq, in_q)))]

    def fetch_act(i):
        slot = lax.rem(i, SLOTS + 1)
        return pltpu.make_async_copy(ha.at[i], w_a.at[slot], sem_act.at[slot])

    @pl.when(first)
    def _():
        for c in range(chunks):
            load_x(0, c).start()

    for copy in weights:
        copy.start()

    @pl.when(first)
    def _():
        def body(i, _):
            for c in range(chunks):
                load_x(i, c).start()
            return 0
        lax.fori_loop(1, micro, body, 0)

    @pl.when(last)
    def _():
        def body(i, _):
            for c in range(chunks):
                load_dy(i, c).start()
            return 0
        lax.fori_loop(0, micro, body, 0)

    barrier = pltpu.get_barrier_semaphore()

    @pl.when(later)
    def _():
        pl.semaphore_signal(barrier, inc=1, device_id={"pp": me - 1}, device_id_type=pl.DeviceIdType.MESH)

    @pl.when(inner)
    def _():
        pl.semaphore_signal(barrier, inc=1, device_id={"pp": me + 1}, device_id_type=pl.DeviceIdType.MESH)

    for copy in weights:
        copy.wait()

    @pl.when(first | last)
    def _():
        pl.semaphore_wait(barrier, 1)

    @pl.when(later & inner)
    def _():
        pl.semaphore_wait(barrier, 2)

    def prepare():
        for n in range(tiles):
            cols = pl.ds(n * COLS, COLS)
            wgt[cols, :] = wg[:, cols].T
            wut[cols, :] = wu[:, cols].T
            wdt[:, cols] = wd[cols, :].T
            acc_g[:, cols] = jnp.zeros((d, COLS), F32)
            acc_u[:, cols] = jnp.zeros((d, COLS), F32)
            acc_d[:, cols] = jnp.zeros((d, COLS), F32)

    @pl.when(later)
    def _():
        prepare()

    def scale_of(wide):
        return lax.rsqrt(jnp.mean(wide * wide, -1, keepdims=True) + EPS)

    def term(i, n, left, right):
        slot = lax.rem(i, SLOTS)
        held = lax.rem(i, SLOTS + 1) if right is w_a else slot
        return dot(left[slot], right[held, :, pl.ds(n * COLS, COLS)]).astype(BF16).astype(F32)

    def weight(i, n, acc, left, right):
        acc[:, pl.ds(n * COLS, COLS)] += term(i, n, left, right)

    def parts(tile_numbers):
        return [(n, *arrays) for n in tile_numbers for arrays in ((acc_g, turned, w_g), (acc_u, turned, w_u), (acc_d, turned_dy, w_a))]

    def forward(i, c, onwards, w):
        fill = [] if w is None else parts([c])
        wide = hs[i, rows(c), :].astype(F32)
        norm[...] = (wide * scale_of(wide)).astype(BF16)
        for part in fill[:2]:
            weight(w, *part)
        for n in range(tiles):
            cols = pl.ds(n * COLS, COLS)
            gate = dot(norm[...], wg[:, cols])
            up = dot(norm[...], wu[:, cols])
            sig = 1.0 / (1.0 + jnp.exp(-gate))
            silu = gate * sig
            slope = up * (sig + silu * (1.0 - sig))
            act = (silu * up).astype(BF16)
            if onwards:
                st_p[c, :, cols] = silu
                st_q[c, :, cols] = slope
                st_a[c, :, cols] = act
            else:
                in_p[c, :, cols] = silu
                in_q[c, :, cols] = slope
                w_a[lax.rem(i, SLOTS + 1), rows(c), cols] = act
        for part in fill[2:]:
            weight(w, *part)
        if onwards:
            out = dot(st_a[c], wd[...]).astype(BF16)
            onward[lax.rem(i, 2), c] = (hs[i, rows(c), :].astype(F32) + out.astype(F32)).astype(BF16)
            send_h(i, c).start()
            for copy in spill(i, c):
                copy.start()

    def backward(i, c, w):
        slot = lax.rem(i, SLOTS)
        each = (tiles - chunks) // chunks
        fill = [] if w is None else parts(range(chunks + c * each, chunks + (c + 1) * each))
        wide = hs[i, rows(c), :].astype(F32)
        scale = scale_of(wide)
        turned[slot, :, rows(c)] = (wide * scale).astype(BF16).T
        turned_dy[slot, :, rows(c)] = ds[i, rows(c), :].T
        for n in range(tiles):
            cols = pl.ds(n * COLS, COLS)
            by_act = dot(ds[i, rows(c), :], wdt[:, cols]).astype(BF16).astype(F32)
            w_g[slot, rows(c), cols] = (by_act * in_q[c, :, cols]).astype(BF16)
            w_u[slot, rows(c), cols] = (by_act * in_p[c, :, cols]).astype(BF16)
        for part in fill[:2]:
            weight(w, *part)
        by_gate = dot(w_g[slot, rows(c), :], wgt[...]).astype(BF16)
        by_up = dot(w_u[slot, rows(c), :], wut[...]).astype(BF16)
        by_a = (by_gate.astype(F32) + by_up.astype(F32)).astype(BF16).astype(F32)
        along = jnp.mean(by_a * wide, -1, keepdims=True) * (scale * scale * scale)
        by_h = (by_a * scale - wide * along).astype(BF16)
        back[c] = (ds[i, rows(c), :].astype(F32) + by_h.astype(F32)).astype(BF16)
        for part in fill[2:]:
            weight(w, *part)

    def step(t, _):
        b = t - ahead
        w = b - (SLOTS - 1)
        has_f, has_b, has_w = t < micro, (b >= 0) & (b < micro), w >= 0
        fetches = inner & (b >= -1) & (b < micro - 1)
        early = (ahead > 2) | (t > micro)

        @pl.when(has_w & inner)
        def _():
            fetch_act(w).wait()

        @pl.when(has_b & inner)
        def _():
            fetch_act(b).start()

        for c in range(chunks):
            @pl.when(has_b)
            def _():
                @pl.when(last)
                def _():
                    load_dy(b, c).wait()

                @pl.when(later & (b > 0))
                def _():
                    send_d(b - 1, c).wait_send()

                @pl.when(inner)
                def _():
                    for copy in fetch(b, c):
                        copy.wait()
                    send_d(b, c).wait_recv()

            @pl.when(has_b & has_w)
            def _():
                backward(b, c, w)

            @pl.when(has_b & jnp.logical_not(has_w))
            def _():
                backward(b, c, None)

            @pl.when(has_b & later)
            def _():
                send_d(b, c).start()

            @pl.when(fetches & early)
            def _():
                for copy in fetch(b + 1, c):
                    copy.start()

        @pl.when(inner & (t > 0) & (t <= micro))
        def _():
            for c in range(chunks):
                for copy in spill(t - 1, c):
                    copy.wait()

        @pl.when(fetches & jnp.logical_not(early))
        def _():
            for c in range(chunks):
                for copy in fetch(b + 1, c):
                    copy.start()

        for c in range(chunks):
            @pl.when(has_f)
            def _():
                @pl.when(first)
                def _():
                    load_x(t, c).wait()

                @pl.when(later)
                def _():
                    send_h(t, c).wait_recv()

                @pl.when(inner & (t > 1))
                def _():
                    send_h(t - 2, c).wait_send()

            for onwards in (True, False):
                at = inner if onwards else last

                @pl.when(has_f & at & has_w)
                def _():
                    forward(t, c, onwards, w)

                @pl.when(has_f & at & jnp.logical_not(has_w))
                def _():
                    forward(t, c, onwards, None)

        @pl.when(first & (t == 0))
        def _():
            prepare()

        @pl.when(has_w & jnp.logical_not(has_f))
        def _():
            for part in parts(range(chunks)):
                weight(w, *part)
        return 0

    lax.fori_loop(0, micro + ahead, step, 0)

    end = micro - 1

    @pl.when(inner)
    def _():
        fetch_act(end).wait()

    free = (micro - 2) % SLOTS
    results = []
    for part in range(2):
        some = range(part * tiles // 2, (part + 1) * tiles // 2)
        for n in some:
            cols = pl.ds(n * COLS, COLS)
            w_g[free, :, cols] = (acc_g[:, cols] + term(end, n, turned, w_g)).astype(BF16)
            w_u[free, :, cols] = (acc_u[:, cols] + term(end, n, turned, w_u)).astype(BF16)
            wd[cols, :] = (acc_d[:, cols] + term(end, n, turned_dy, w_a)).astype(BF16).T
        span = pl.ds(some[0] * COLS, len(some) * COLS)
        copies = [pltpu.make_async_copy(w_g.at[free, :, span], og.at[0, :, span], sem_out.at[0, part]),
                  pltpu.make_async_copy(w_u.at[free, :, span], ou.at[0, :, span], sem_out.at[1, part]),
                  pltpu.make_async_copy(wd.at[span], od.at[0, span], sem_out.at[2, part])]
        for copy in copies:
            copy.start()
        results += copies

    @pl.when(later)
    def _():
        for c in range(chunks):
            send_d(end, c).wait_send()

    @pl.when(inner)
    def _():
        for c in range(chunks):
            send_h(micro - 2, c).wait_send()
            send_h(micro - 1, c).wait_send()

    for copy in results:
        copy.wait()


def hand_over(*refs):
    sources, results, held, sem_in, sem_out = refs[:3], refs[3:6], refs[6:9], refs[9], refs[10]
    reads = [pltpu.make_async_copy(a, b, sem_in.at[i]) for i, (a, b) in enumerate(zip(sources, held, strict=True))]
    writes = [pltpu.make_async_copy(a, b, sem_out.at[i]) for i, (a, b) in enumerate(zip(held, results, strict=True))]
    for copy in reads:
        copy.start()
    for read, write in zip(reads, writes, strict=True):
        read.wait()
        write.start()
    for copy in writes:
        copy.wait()


def solution(mesh):
    stages = mesh.shape["pp"]

    def step(x, dy, w_gate, w_up, w_down):
        micro, tokens, d = x.shape
        ff = w_gate.shape[-1]
        chunks = tokens // ROWS
        hbm = pl.BlockSpec(memory_space=pl.ANY)
        vmem, dma = pltpu.VMEM, pltpu.SemaphoreType.DMA
        outs = pl.pallas_call(
            functools.partial(kernel, stages),
            out_shape=[
                jax.ShapeDtypeStruct(w_gate.shape, BF16),
                jax.ShapeDtypeStruct(w_up.shape, BF16),
                jax.ShapeDtypeStruct(w_down.shape, BF16),
                jax.ShapeDtypeStruct((micro, tokens, ff), F32),
                jax.ShapeDtypeStruct((micro, tokens, ff), F32),
                jax.ShapeDtypeStruct((micro, tokens, ff), BF16),
            ],
            in_specs=[hbm] * 5,
            out_specs=[hbm] * 6,
            scratch_shapes=[
                vmem((d, ff), BF16), vmem((d, ff), BF16), vmem((ff, d), BF16),
                vmem((ff, d), BF16), vmem((ff, d), BF16), vmem((d, ff), BF16),
                vmem((d, ff), F32), vmem((d, ff), F32), vmem((d, ff), F32),
                vmem((micro, tokens, d), BF16), vmem((micro, tokens, d), BF16),
                vmem((ROWS, d), BF16), vmem((SLOTS, d, tokens), BF16), vmem((SLOTS, d, tokens), BF16),
                vmem((chunks, ROWS, ff), F32), vmem((chunks, ROWS, ff), F32), vmem((chunks, ROWS, ff), BF16),
                vmem((chunks, ROWS, ff), F32), vmem((chunks, ROWS, ff), F32),
                vmem((SLOTS + 1, tokens, ff), BF16), vmem((SLOTS, tokens, ff), BF16), vmem((SLOTS, tokens, ff), BF16),
                vmem((2, chunks, ROWS, d), BF16), vmem((chunks, ROWS, d), BF16),
                dma((3,)), dma((micro, chunks)), dma((micro, chunks)), dma((2, chunks)), dma((chunks,)),
                dma((3, chunks)), dma((2, chunks)), dma((SLOTS + 1,)), dma((3, 2)),
            ],
            compiler_params=pltpu.CompilerParams(collective_id=0, has_side_effects=True, vmem_limit_bytes=67000000),
        )(x, dy, w_gate, w_up, w_down)
        shapes = [jax.ShapeDtypeStruct(w.shape, BF16) for w in (w_gate, w_up, w_down)]
        return tuple(pl.pallas_call(
            hand_over,
            out_shape=shapes,
            in_specs=[hbm] * 3,
            out_specs=[hbm] * 3,
            scratch_shapes=[vmem(a.shape, a.dtype) for a in shapes] + [dma((3,)), dma((3,))],
        )(*outs[:3]))

    return jax.shard_map(
        step,
        mesh=mesh,
        in_specs=(P("rep", None, None),) * 2 + (P("pp", None, None),) * 3,
        out_specs=(P(("rep", "pp"), None, None),) * 3,
        check_vma=False,
    )
```

```python
import functools

import jax
import jax.numpy as jnp
from jax import lax
from jax.experimental import pallas as pl
from jax.experimental.pallas import tpu as pltpu
from jax.sharding import PartitionSpec as P

F32, BF16 = jnp.float32, jnp.bfloat16
ROWS = 256
COLS = 256
EPS = 1e-6


LEAD = (1, 2, 5, 6, 9, 10, 15, 16)
LAG = (8, 8, 6, 8, 3, 2, 2, 2)


def at_stage(table, stages, me):
    number = 0
    for stage in range(stages):
        number = jnp.where(me == stage, table[min(stages - 1 - stage, len(table) - 1)], number)
    return number


def dot(a, b):
    return jnp.dot(a, b, preferred_element_type=F32)


def kernel(stages, x, dy, wg_in, wu_in, wd_in, og, ou, od, hp, hq, ha, hg, hu,
           wg, wu, wd, wgt, wut, wdt, acc_g, acc_u, acc_d, hs, ds, norm, turned, turned_dy,
           st_p, st_q, st_a, st_g, st_u, in_p, in_q, w_a, w_g, w_u, onward, back,
           sem_w, sem_h, sem_d, sem_f, sem_b, sem_st, sem_by, sem_in, sem_wt, sem_out):
    micro, tokens, d = x.shape
    ff = wg_in.shape[-1]
    chunks, tiles = tokens // ROWS, ff // COLS
    me = lax.axis_index("pp")
    first, last = me == 0, me == stages - 1
    inner = jnp.logical_not(last)
    later = jnp.logical_not(first)
    ahead, lag = at_stage(LEAD, stages, me), at_stage(LAG, stages, me)

    weights = [pltpu.make_async_copy(src.at[0], dst, sem_w.at[i]) for i, (src, dst) in enumerate(((wg_in, wg), (wu_in, wu), (wd_in, wd)))]

    def rows(c):
        return pl.ds(c * ROWS, ROWS)

    def load_x(i, c):
        return pltpu.make_async_copy(x.at[i, rows(c)], hs.at[i, rows(c)], sem_h.at[i, c])

    def load_dy(i, c):
        return pltpu.make_async_copy(dy.at[i, rows(c)], ds.at[i, rows(c)], sem_d.at[i, c])

    def send_h(i, c):
        slot = lax.rem(i, 2)
        return pltpu.make_async_remote_copy(onward.at[slot, c], hs.at[i, rows(c)], sem_f.at[slot, c], sem_h.at[i, c],
                                            device_id={"pp": me + 1}, device_id_type=pl.DeviceIdType.MESH)

    def send_d(i, c):
        return pltpu.make_async_remote_copy(back.at[c], ds.at[i, rows(c)], sem_b.at[c], sem_d.at[i, c],
                                            device_id={"pp": me - 1}, device_id_type=pl.DeviceIdType.MESH)

    def spill_act(i, c):
        return pltpu.make_async_copy(st_a.at[c], ha.at[i, rows(c)], sem_st.at[2, c])

    def spill(i, c):
        return [pltpu.make_async_copy(src.at[c], dst.at[i, rows(c)], sem_st.at[k, c]) for k, (src, dst) in enumerate(((st_p, hp), (st_q, hq)))]

    def spill_by(i, c):
        return [pltpu.make_async_copy(src.at[c], dst.at[i, rows(c)], sem_by.at[k, c]) for k, (src, dst) in enumerate(((st_g, hg), (st_u, hu)))]

    def fetch(i, c):
        return [pltpu.make_async_copy(src.at[i, rows(c)], dst.at[c], sem_in.at[k, c])
                for k, (src, dst) in enumerate(((hp, in_p), (hq, in_q)))]

    each = (tiles - chunks) // chunks
    groups = [range(chunks + c * each, chunks + (c + 1) * each) for c in range(chunks)] + [range(chunks)]

    def fetch_tiles(i, group):
        span = pl.ds(groups[group][0] * COLS, len(groups[group]) * COLS)
        return [pltpu.make_async_copy(src.at[i, :, span], dst.at[:, span], sem_wt.at[k, group])
                for k, (src, dst) in enumerate(((hg, w_g), (hu, w_u), (ha, w_a)))]

    @pl.when(first)
    def _():
        for c in range(chunks):
            load_x(0, c).start()

    for copy in weights:
        copy.start()

    @pl.when(first)
    def _():
        def body(i, _):
            for c in range(chunks):
                load_x(i, c).start()
            return 0
        lax.fori_loop(1, micro, body, 0)

    @pl.when(last)
    def _():
        def body(i, _):
            for c in range(chunks):
                load_dy(i, c).start()
            return 0
        lax.fori_loop(0, micro, body, 0)

    barrier = pltpu.get_barrier_semaphore()

    @pl.when(later)
    def _():
        pl.semaphore_signal(barrier, inc=1, device_id={"pp": me - 1}, device_id_type=pl.DeviceIdType.MESH)

    @pl.when(inner)
    def _():
        pl.semaphore_signal(barrier, inc=1, device_id={"pp": me + 1}, device_id_type=pl.DeviceIdType.MESH)

    for copy in weights:
        copy.wait()

    @pl.when(first | last)
    def _():
        pl.semaphore_wait(barrier, 1)

    @pl.when(later & inner)
    def _():
        pl.semaphore_wait(barrier, 2)

    def prepare():
        for n in range(tiles):
            cols = pl.ds(n * COLS, COLS)
            wgt[cols, :] = wg[:, cols].T
            wut[cols, :] = wu[:, cols].T
            wdt[:, cols] = wd[cols, :].T
            acc_g[:, cols] = jnp.zeros((d, COLS), F32)
            acc_u[:, cols] = jnp.zeros((d, COLS), F32)
            acc_d[:, cols] = jnp.zeros((d, COLS), F32)

    @pl.when(later)
    def _():
        prepare()

    def scale_of(wide):
        return lax.rsqrt(jnp.mean(wide * wide, -1, keepdims=True) + EPS)

    def term(i, n, left, right):
        return dot(left[lax.rem(i, 2)], right[:, pl.ds(n * COLS, COLS)]).astype(BF16).astype(F32)

    def weight(i, n, acc, left, right):
        acc[:, pl.ds(n * COLS, COLS)] += term(i, n, left, right)

    def turn(i, c):
        i = jnp.clip(i, 0, micro - 1)
        wide = hs[i, rows(c), :].astype(F32)
        turned[lax.rem(i, 2), :, rows(c)] = (wide * scale_of(wide)).astype(BF16).T
        turned_dy[lax.rem(i, 2), :, rows(c)] = ds[i, rows(c), :].T

    def parts(tile_numbers):
        return [(n, *arrays) for n in tile_numbers for arrays in ((acc_g, turned, w_g), (acc_u, turned, w_u), (acc_d, turned_dy, w_a))]

    def forward(i, c, onwards, w):
        fill = [] if w is None else parts([c])
        wide = hs[i, rows(c), :].astype(F32)
        norm[...] = (wide * scale_of(wide)).astype(BF16)
        for part in fill[:2]:
            weight(w, *part)
        for n in range(tiles):
            cols = pl.ds(n * COLS, COLS)
            gate = dot(norm[...], wg[:, cols])
            up = dot(norm[...], wu[:, cols])
            sig = 1.0 / (1.0 + jnp.exp(-gate))
            silu = gate * sig
            slope = up * (sig + silu * (1.0 - sig))
            act = (silu * up).astype(BF16)
            if onwards:
                st_p[c, :, cols] = silu
                st_q[c, :, cols] = slope
            else:
                in_p[c, :, cols] = silu
                in_q[c, :, cols] = slope
            st_a[c, :, cols] = act
        for part in fill[2:]:
            weight(w, *part)
        if onwards:
            out = dot(st_a[c], wd[...]).astype(BF16)
            onward[lax.rem(i, 2), c] = (hs[i, rows(c), :].astype(F32) + out.astype(F32)).astype(BF16)
            send_h(i, c).start()
            for copy in spill(i, c):
                copy.start()
        spill_act(i, c).start()

    def backward(i, c, w, upcoming):
        fill = [] if w is None else parts(groups[c])
        wide = hs[i, rows(c), :].astype(F32)
        scale = scale_of(wide)
        turn(upcoming, c)
        for n in range(tiles):
            cols = pl.ds(n * COLS, COLS)
            by_act = dot(ds[i, rows(c), :], wdt[:, cols]).astype(BF16).astype(F32)
            st_g[c, :, cols] = (by_act * in_q[c, :, cols]).astype(BF16)
            st_u[c, :, cols] = (by_act * in_p[c, :, cols]).astype(BF16)
        for part in fill[:2]:
            weight(w, *part)
        by_gate = dot(st_g[c], wgt[...]).astype(BF16)
        by_up = dot(st_u[c], wut[...]).astype(BF16)
        by_a = (by_gate.astype(F32) + by_up.astype(F32)).astype(BF16).astype(F32)
        along = jnp.mean(by_a * wide, -1, keepdims=True) * (scale * scale * scale)
        by_h = (by_a * scale - wide * along).astype(BF16)
        back[c] = (ds[i, rows(c), :].astype(F32) + by_h.astype(F32)).astype(BF16)
        for part in fill[2:]:
            weight(w, *part)

    def step(t, _):
        b = t - ahead
        w = b - lag
        has_f, has_b, has_w = t < micro, (b >= 0) & (b < micro), w >= 0
        fetches = inner & (b >= -1) & (b < micro - 1)
        early = (ahead > 2) | (t > micro)
        next_w = w >= -1

        def refill(group):
            @pl.when(next_w)
            def _():
                for copy in fetch_tiles(w + 1, group):
                    copy.start()

        def ready(some):
            @pl.when(has_w)
            def _():
                for group in some:
                    for copy in fetch_tiles(w, group):
                        copy.wait()

        ready(range(chunks))

        @pl.when((b > 0) & (b <= micro))
        def _():
            for c in range(chunks):
                for copy in spill_by(b - 1, c):
                    copy.wait()

        for c in range(chunks):
            @pl.when(has_b)
            def _():
                @pl.when(last)
                def _():
                    load_dy(b, c).wait()

                @pl.when(later & (b > 0))
                def _():
                    send_d(b - 1, c).wait_send()

                @pl.when(inner)
                def _():
                    for copy in fetch(b, c):
                        copy.wait()
                    send_d(b, c).wait_recv()

            @pl.when(has_b & has_w)
            def _():
                backward(b, c, w, w + 1)

            @pl.when(has_b & jnp.logical_not(has_w))
            def _():
                backward(b, c, None, w + 1)

            @pl.when(has_b & later)
            def _():
                send_d(b, c).start()

            @pl.when(has_b)
            def _():
                for copy in spill_by(b, c):
                    copy.start()

            @pl.when(fetches & early)
            def _():
                for copy in fetch(b + 1, c):
                    copy.start()

        @pl.when(has_w & jnp.logical_not(has_b))
        def _():
            for c in range(chunks):
                turn(w + 1, c)
            for part in parts(range(chunks, tiles)):
                weight(w, *part)

        for group in range(chunks):
            refill(group)
        ready([chunks])

        @pl.when((t > 0) & (t <= micro))
        def _():
            for c in range(chunks):
                spill_act(t - 1, c).wait()

        @pl.when(inner & (t > 0) & (t <= micro))
        def _():
            for c in range(chunks):
                for copy in spill(t - 1, c):
                    copy.wait()

        @pl.when(fetches & jnp.logical_not(early))
        def _():
            for c in range(chunks):
                for copy in fetch(b + 1, c):
                    copy.start()

        for c in range(chunks):
            @pl.when(has_f)
            def _():
                @pl.when(first)
                def _():
                    load_x(t, c).wait()

                @pl.when(later)
                def _():
                    send_h(t, c).wait_recv()

                @pl.when(inner & (t > 1))
                def _():
                    send_h(t - 2, c).wait_send()

            for onwards in (True, False):
                at = inner if onwards else last

                @pl.when(has_f & at & has_w)
                def _():
                    forward(t, c, onwards, w)

                @pl.when(has_f & at & jnp.logical_not(has_w))
                def _():
                    forward(t, c, onwards, None)

        @pl.when(first & (t == 0))
        def _():
            prepare()

        @pl.when(has_w & jnp.logical_not(has_f))
        def _():
            for part in parts(range(chunks)):
                weight(w, *part)

        refill(chunks)
        return 0

    lax.fori_loop(0, micro + ahead + lag - 1, step, 0)

    end = micro - 1

    for group in range(chunks + 1):
        for copy in fetch_tiles(end, group):
            copy.wait()
    results = []
    for part in range(2):
        some = range(part * tiles // 2, (part + 1) * tiles // 2)
        for n in some:
            cols = pl.ds(n * COLS, COLS)
            wg[:, cols] = (acc_g[:, cols] + term(end, n, turned, w_g)).astype(BF16)
            wu[:, cols] = (acc_u[:, cols] + term(end, n, turned, w_u)).astype(BF16)
            wd[cols, :] = (acc_d[:, cols] + term(end, n, turned_dy, w_a)).astype(BF16).T
        span = pl.ds(some[0] * COLS, len(some) * COLS)
        copies = [pltpu.make_async_copy(wg.at[:, span], og.at[0, :, span], sem_out.at[0, part]),
                  pltpu.make_async_copy(wu.at[:, span], ou.at[0, :, span], sem_out.at[1, part]),
                  pltpu.make_async_copy(wd.at[span], od.at[0, span], sem_out.at[2, part])]
        for copy in copies:
            copy.start()
        results += copies

    @pl.when(later)
    def _():
        for c in range(chunks):
            send_d(end, c).wait_send()

    @pl.when(inner)
    def _():
        for c in range(chunks):
            send_h(micro - 2, c).wait_send()
            send_h(micro - 1, c).wait_send()

    for copy in results:
        copy.wait()


def hand_over(*refs):
    sources, results, held, sem_in, sem_out = refs[:3], refs[3:6], refs[6:9], refs[9], refs[10]
    reads = [pltpu.make_async_copy(a, b, sem_in.at[i]) for i, (a, b) in enumerate(zip(sources, held, strict=True))]
    writes = [pltpu.make_async_copy(a, b, sem_out.at[i]) for i, (a, b) in enumerate(zip(held, results, strict=True))]
    for copy in reads:
        copy.start()
    for read, write in zip(reads, writes, strict=True):
        read.wait()
        write.start()
    for copy in writes:
        copy.wait()


def solution(mesh):
    stages = mesh.shape["pp"]

    def step(x, dy, w_gate, w_up, w_down):
        micro, tokens, d = x.shape
        ff = w_gate.shape[-1]
        chunks = tokens // ROWS
        hbm = pl.BlockSpec(memory_space=pl.ANY)
        vmem, dma = pltpu.VMEM, pltpu.SemaphoreType.DMA
        outs = pl.pallas_call(
            functools.partial(kernel, stages),
            out_shape=[
                jax.ShapeDtypeStruct(w_gate.shape, BF16),
                jax.ShapeDtypeStruct(w_up.shape, BF16),
                jax.ShapeDtypeStruct(w_down.shape, BF16),
                jax.ShapeDtypeStruct((micro, tokens, ff), F32),
                jax.ShapeDtypeStruct((micro, tokens, ff), F32),
                jax.ShapeDtypeStruct((micro, tokens, ff), BF16),
                jax.ShapeDtypeStruct((micro, tokens, ff), BF16),
                jax.ShapeDtypeStruct((micro, tokens, ff), BF16),
            ],
            in_specs=[hbm] * 5,
            out_specs=[hbm] * 8,
            scratch_shapes=[
                vmem((d, ff), BF16), vmem((d, ff), BF16), vmem((ff, d), BF16),
                vmem((ff, d), BF16), vmem((ff, d), BF16), vmem((d, ff), BF16),
                vmem((d, ff), F32), vmem((d, ff), F32), vmem((d, ff), F32),
                vmem((micro, tokens, d), BF16), vmem((micro, tokens, d), BF16),
                vmem((ROWS, d), BF16), vmem((2, d, tokens), BF16), vmem((2, d, tokens), BF16),
                vmem((chunks, ROWS, ff), F32), vmem((chunks, ROWS, ff), F32),
                vmem((chunks, ROWS, ff), BF16), vmem((chunks, ROWS, ff), BF16), vmem((chunks, ROWS, ff), BF16),
                vmem((chunks, ROWS, ff), F32), vmem((chunks, ROWS, ff), F32),
                vmem((tokens, ff), BF16), vmem((tokens, ff), BF16), vmem((tokens, ff), BF16),
                vmem((2, chunks, ROWS, d), BF16), vmem((chunks, ROWS, d), BF16),
                dma((3,)), dma((micro, chunks)), dma((micro, chunks)), dma((2, chunks)), dma((chunks,)),
                dma((3, chunks)), dma((2, chunks)), dma((2, chunks)), dma((3, chunks + 1)), dma((3, 2)),
            ],
            compiler_params=pltpu.CompilerParams(collective_id=0, has_side_effects=True, vmem_limit_bytes=67000000),
        )(x, dy, w_gate, w_up, w_down)
        shapes = [jax.ShapeDtypeStruct(w.shape, BF16) for w in (w_gate, w_up, w_down)]
        return tuple(pl.pallas_call(
            hand_over,
            out_shape=shapes,
            in_specs=[hbm] * 3,
            out_specs=[hbm] * 3,
            scratch_shapes=[vmem(a.shape, a.dtype) for a in shapes] + [dma((3,)), dma((3,))],
        )(*outs[:3]))

    return jax.shard_map(
        step,
        mesh=mesh,
        in_specs=(P("rep", None, None),) * 2 + (P("pp", None, None),) * 3,
        out_specs=(P(("rep", "pp"), None, None),) * 3,
        check_vma=False,
    )
```

```python
import functools

import jax
import jax.numpy as jnp
from jax import lax
from jax.experimental import pallas as pl
from jax.experimental.pallas import tpu as pltpu
from jax.sharding import PartitionSpec as P

F32, BF16 = jnp.float32, jnp.bfloat16
ROWS = 256
COLS = 256
EPS = 1e-6


LEAD = (1, 2, 5, 6, 9, 10, 15, 16)
LAG = (10, 10, 8, 8, 4, 3, 2, 2)


def at_stage(table, stages, me):
    number = 0
    for stage in range(stages):
        number = jnp.where(me == stage, table[min(stages - 1 - stage, len(table) - 1)], number)
    return number


def dot(a, b):
    return jnp.dot(a, b, preferred_element_type=F32)


def kernel(stages, x, dy, wg_in, wu_in, wd_in, og, ou, od, hp, hq, ha, hg, hu,
           wg, wu, wd, wgt, wut, wdt, acc_g, acc_u, acc_d, hs, ds, norm, turned, turned_dy,
           st_p, st_q, st_a, st_g, st_u, in_p, in_q, w_a, w_g, w_u, onward, back,
           sem_w, sem_h, sem_d, sem_f, sem_b, sem_st, sem_by, sem_in, sem_wt, sem_out):
    micro, tokens, d = x.shape
    ff = wg_in.shape[-1]
    chunks, tiles = tokens // ROWS, ff // COLS
    me = lax.axis_index("pp")
    first, last = me == 0, me == stages - 1
    inner = jnp.logical_not(last)
    later = jnp.logical_not(first)
    ahead, lag = at_stage(LEAD, stages, me), at_stage(LAG, stages, me)

    weights = [pltpu.make_async_copy(src.at[0], dst, sem_w.at[i]) for i, (src, dst) in enumerate(((wg_in, wg), (wu_in, wu), (wd_in, wd)))]

    def rows(c):
        return pl.ds(c * ROWS, ROWS)

    def load_x(i, c):
        return pltpu.make_async_copy(x.at[i, rows(c)], hs.at[i, rows(c)], sem_h.at[i, c])

    def load_dy(i, c):
        return pltpu.make_async_copy(dy.at[i, rows(c)], ds.at[i, rows(c)], sem_d.at[i, c])

    def send_h(i, c):
        slot = lax.rem(i, 2)
        return pltpu.make_async_remote_copy(onward.at[slot, c], hs.at[i, rows(c)], sem_f.at[slot, c], sem_h.at[i, c],
                                            device_id={"pp": me + 1}, device_id_type=pl.DeviceIdType.MESH)

    def send_d(i, c):
        return pltpu.make_async_remote_copy(back.at[c], ds.at[i, rows(c)], sem_b.at[c], sem_d.at[i, c],
                                            device_id={"pp": me - 1}, device_id_type=pl.DeviceIdType.MESH)

    def spill_act(i, c):
        return pltpu.make_async_copy(st_a.at[c], ha.at[i, rows(c)], sem_st.at[2, c])

    def spill(i, c):
        return [pltpu.make_async_copy(src.at[c], dst.at[i, rows(c)], sem_st.at[k, c]) for k, (src, dst) in enumerate(((st_p, hp), (st_q, hq)))]

    def spill_by(i, c):
        return [pltpu.make_async_copy(src.at[c], dst.at[i, rows(c)], sem_by.at[k, c]) for k, (src, dst) in enumerate(((st_g, hg), (st_u, hu)))]

    def fetch(i, c):
        return [pltpu.make_async_copy(src.at[i, rows(c)], dst.at[c], sem_in.at[k, c])
                for k, (src, dst) in enumerate(((hp, in_p), (hq, in_q)))]

    each = (tiles - chunks) // chunks
    groups = [range(chunks + c * each, chunks + (c + 1) * each) for c in range(chunks)] + [range(chunks)]

    def fetch_tiles(i, group):
        span = pl.ds(groups[group][0] * COLS, len(groups[group]) * COLS)
        return [pltpu.make_async_copy(src.at[i, :, span], dst.at[:, span], sem_wt.at[k, group])
                for k, (src, dst) in enumerate(((hg, w_g), (hu, w_u), (ha, w_a)))]

    @pl.when(first)
    def _():
        for c in range(chunks):
            load_x(0, c).start()

    for copy in weights:
        copy.start()

    @pl.when(first)
    def _():
        def body(i, _):
            for c in range(chunks):
                load_x(i, c).start()
            return 0
        lax.fori_loop(1, micro, body, 0)

    @pl.when(last)
    def _():
        def body(i, _):
            for c in range(chunks):
                load_dy(i, c).start()
            return 0
        lax.fori_loop(0, micro, body, 0)

    barrier = pltpu.get_barrier_semaphore()

    @pl.when(later)
    def _():
        pl.semaphore_signal(barrier, inc=1, device_id={"pp": me - 1}, device_id_type=pl.DeviceIdType.MESH)

    @pl.when(inner)
    def _():
        pl.semaphore_signal(barrier, inc=1, device_id={"pp": me + 1}, device_id_type=pl.DeviceIdType.MESH)

    for copy in weights:
        copy.wait()

    @pl.when(first | last)
    def _():
        pl.semaphore_wait(barrier, 1)

    @pl.when(later & inner)
    def _():
        pl.semaphore_wait(barrier, 2)

    def prepare():
        for n in range(tiles):
            cols = pl.ds(n * COLS, COLS)
            wgt[cols, :] = wg[:, cols].T
            wut[cols, :] = wu[:, cols].T
            wdt[:, cols] = wd[cols, :].T
            acc_g[:, cols] = jnp.zeros((d, COLS), F32)
            acc_u[:, cols] = jnp.zeros((d, COLS), F32)
            acc_d[:, cols] = jnp.zeros((d, COLS), F32)

    @pl.when(later)
    def _():
        prepare()

    def scale_of(wide):
        return lax.rsqrt(jnp.mean(wide * wide, -1, keepdims=True) + EPS)

    def term(i, n, left, right):
        return dot(left[lax.rem(i, 2)], right[:, pl.ds(n * COLS, COLS)]).astype(BF16).astype(F32)

    def weight(i, n, acc, left, right):
        acc[:, pl.ds(n * COLS, COLS)] += term(i, n, left, right)

    def turn(i, c):
        i = jnp.clip(i, 0, micro - 1)
        wide = hs[i, rows(c), :].astype(F32)
        turned[lax.rem(i, 2), :, rows(c)] = (wide * scale_of(wide)).astype(BF16).T
        turned_dy[lax.rem(i, 2), :, rows(c)] = ds[i, rows(c), :].T

    def parts(tile_numbers):
        return [(n, *arrays) for n in tile_numbers for arrays in ((acc_g, turned, w_g), (acc_u, turned, w_u), (acc_d, turned_dy, w_a))]

    def forward(i, c, onwards, w):
        fill = [] if w is None else parts([c])
        wide = hs[i, rows(c), :].astype(F32)
        norm[...] = (wide * scale_of(wide)).astype(BF16)
        for part in fill[:2]:
            weight(w, *part)
        for n in range(tiles):
            cols = pl.ds(n * COLS, COLS)
            gate = dot(norm[...], wg[:, cols])
            up = dot(norm[...], wu[:, cols])
            sig = 1.0 / (1.0 + jnp.exp(-gate))
            silu = gate * sig
            slope = up * (sig + silu * (1.0 - sig))
            act = (silu * up).astype(BF16)
            if onwards:
                st_p[c, :, cols] = silu
                st_q[c, :, cols] = slope
            else:
                in_p[c, :, cols] = silu
                in_q[c, :, cols] = slope
            st_a[c, :, cols] = act
        for part in fill[2:]:
            weight(w, *part)
        if onwards:
            out = dot(st_a[c], wd[...]).astype(BF16)
            onward[lax.rem(i, 2), c] = (hs[i, rows(c), :].astype(F32) + out.astype(F32)).astype(BF16)
            send_h(i, c).start()
            for copy in spill(i, c):
                copy.start()
        spill_act(i, c).start()

    def backward(i, c, w, upcoming):
        fill = [] if w is None else parts(groups[c])
        wide = hs[i, rows(c), :].astype(F32)
        scale = scale_of(wide)
        turn(upcoming, c)
        for n in range(tiles):
            cols = pl.ds(n * COLS, COLS)
            by_act = dot(ds[i, rows(c), :], wdt[:, cols]).astype(BF16).astype(F32)
            st_g[c, :, cols] = (by_act * in_q[c, :, cols]).astype(BF16)
            st_u[c, :, cols] = (by_act * in_p[c, :, cols]).astype(BF16)
        for part in fill[:2]:
            weight(w, *part)
        by_gate = dot(st_g[c], wgt[...]).astype(BF16)
        by_up = dot(st_u[c], wut[...]).astype(BF16)
        by_a = (by_gate.astype(F32) + by_up.astype(F32)).astype(BF16).astype(F32)
        along = jnp.mean(by_a * wide, -1, keepdims=True) * (scale * scale * scale)
        by_h = (by_a * scale - wide * along).astype(BF16)
        back[c] = (ds[i, rows(c), :].astype(F32) + by_h.astype(F32)).astype(BF16)
        for part in fill[2:]:
            weight(w, *part)

    def step(t, _):
        b = t - ahead
        w = b - lag
        has_f, has_b, has_w = t < micro, (b >= 0) & (b < micro), w >= 0
        fetches = inner & (b >= -1) & (b < micro - 1)
        next_w = w >= -1

        def refill(group):
            @pl.when(next_w)
            def _():
                for copy in fetch_tiles(w + 1, group):
                    copy.start()

        def ready(some):
            @pl.when(has_w)
            def _():
                for group in some:
                    for copy in fetch_tiles(w, group):
                        copy.wait()

        @pl.when((b > 0) & (b <= micro))
        def _():
            for c in range(chunks):
                for copy in spill_by(b - 1, c):
                    copy.wait()

        for c in range(chunks):
            ready([c])

            @pl.when(has_b)
            def _():
                @pl.when(last)
                def _():
                    load_dy(b, c).wait()

                @pl.when(later & (b > 0))
                def _():
                    send_d(b - 1, c).wait_send()

                @pl.when(inner)
                def _():
                    for copy in fetch(b, c):
                        copy.wait()
                    send_d(b, c).wait_recv()

            @pl.when(has_b & has_w)
            def _():
                backward(b, c, w, w + 1)

            @pl.when(has_b & jnp.logical_not(has_w))
            def _():
                backward(b, c, None, w + 1)

            @pl.when(has_w & jnp.logical_not(has_b))
            def _():
                turn(w + 1, c)
                for part in parts(groups[c]):
                    weight(w, *part)

            @pl.when(has_b & later)
            def _():
                send_d(b, c).start()

            @pl.when(has_b)
            def _():
                for copy in spill_by(b, c):
                    copy.start()

            @pl.when((t > 0) & (t <= micro))
            def _():
                spill_act(t - 1, c).wait()

            @pl.when(inner & (t > 0) & (t <= micro))
            def _():
                for copy in spill(t - 1, c):
                    copy.wait()

            @pl.when(fetches)
            def _():
                for copy in fetch(b + 1, c):
                    copy.start()

            refill(c)

        ready([chunks])

        for c in range(chunks):
            @pl.when(has_f)
            def _():
                @pl.when(first)
                def _():
                    load_x(t, c).wait()

                @pl.when(later)
                def _():
                    send_h(t, c).wait_recv()

                @pl.when(inner & (t > 1))
                def _():
                    send_h(t - 2, c).wait_send()

            for onwards in (True, False):
                at = inner if onwards else last

                @pl.when(has_f & at & has_w)
                def _():
                    forward(t, c, onwards, w)

                @pl.when(has_f & at & jnp.logical_not(has_w))
                def _():
                    forward(t, c, onwards, None)

        @pl.when(first & (t == 0))
        def _():
            prepare()

        @pl.when(has_w & jnp.logical_not(has_f))
        def _():
            for part in parts(range(chunks)):
                weight(w, *part)

        refill(chunks)
        return 0

    lax.fori_loop(0, micro + ahead + lag - 1, step, 0)

    end = micro - 1

    for group in range(chunks + 1):
        for copy in fetch_tiles(end, group):
            copy.wait()
    results = []
    for part in range(2):
        some = range(part * tiles // 2, (part + 1) * tiles // 2)
        for n in some:
            cols = pl.ds(n * COLS, COLS)
            wg[:, cols] = (acc_g[:, cols] + term(end, n, turned, w_g)).astype(BF16)
            wu[:, cols] = (acc_u[:, cols] + term(end, n, turned, w_u)).astype(BF16)
            wd[cols, :] = (acc_d[:, cols] + term(end, n, turned_dy, w_a)).astype(BF16).T
        span = pl.ds(some[0] * COLS, len(some) * COLS)
        copies = [pltpu.make_async_copy(wg.at[:, span], og.at[0, :, span], sem_out.at[0, part]),
                  pltpu.make_async_copy(wu.at[:, span], ou.at[0, :, span], sem_out.at[1, part]),
                  pltpu.make_async_copy(wd.at[span], od.at[0, span], sem_out.at[2, part])]
        for copy in copies:
            copy.start()
        results += copies

    @pl.when(later)
    def _():
        for c in range(chunks):
            send_d(end, c).wait_send()

    @pl.when(inner)
    def _():
        for c in range(chunks):
            send_h(micro - 2, c).wait_send()
            send_h(micro - 1, c).wait_send()

    for copy in results:
        copy.wait()


def hand_over(*refs):
    sources, results, held, sem_in, sem_out = refs[:3], refs[3:6], refs[6:9], refs[9], refs[10]
    reads = [pltpu.make_async_copy(a, b, sem_in.at[i]) for i, (a, b) in enumerate(zip(sources, held, strict=True))]
    writes = [pltpu.make_async_copy(a, b, sem_out.at[i]) for i, (a, b) in enumerate(zip(held, results, strict=True))]
    for copy in reads:
        copy.start()
    for read, write in zip(reads, writes, strict=True):
        read.wait()
        write.start()
    for copy in writes:
        copy.wait()


def solution(mesh):
    stages = mesh.shape["pp"]

    def step(x, dy, w_gate, w_up, w_down):
        micro, tokens, d = x.shape
        ff = w_gate.shape[-1]
        chunks = tokens // ROWS
        hbm = pl.BlockSpec(memory_space=pl.ANY)
        vmem, dma = pltpu.VMEM, pltpu.SemaphoreType.DMA
        outs = pl.pallas_call(
            functools.partial(kernel, stages),
            out_shape=[
                jax.ShapeDtypeStruct(w_gate.shape, BF16),
                jax.ShapeDtypeStruct(w_up.shape, BF16),
                jax.ShapeDtypeStruct(w_down.shape, BF16),
                jax.ShapeDtypeStruct((micro, tokens, ff), F32),
                jax.ShapeDtypeStruct((micro, tokens, ff), F32),
                jax.ShapeDtypeStruct((micro, tokens, ff), BF16),
                jax.ShapeDtypeStruct((micro, tokens, ff), BF16),
                jax.ShapeDtypeStruct((micro, tokens, ff), BF16),
            ],
            in_specs=[hbm] * 5,
            out_specs=[hbm] * 8,
            scratch_shapes=[
                vmem((d, ff), BF16), vmem((d, ff), BF16), vmem((ff, d), BF16),
                vmem((ff, d), BF16), vmem((ff, d), BF16), vmem((d, ff), BF16),
                vmem((d, ff), F32), vmem((d, ff), F32), vmem((d, ff), F32),
                vmem((micro, tokens, d), BF16), vmem((micro, tokens, d), BF16),
                vmem((ROWS, d), BF16), vmem((2, d, tokens), BF16), vmem((2, d, tokens), BF16),
                vmem((chunks, ROWS, ff), F32), vmem((chunks, ROWS, ff), F32),
                vmem((chunks, ROWS, ff), BF16), vmem((chunks, ROWS, ff), BF16), vmem((chunks, ROWS, ff), BF16),
                vmem((chunks, ROWS, ff), F32), vmem((chunks, ROWS, ff), F32),
                vmem((tokens, ff), BF16), vmem((tokens, ff), BF16), vmem((tokens, ff), BF16),
                vmem((2, chunks, ROWS, d), BF16), vmem((chunks, ROWS, d), BF16),
                dma((3,)), dma((micro, chunks)), dma((micro, chunks)), dma((2, chunks)), dma((chunks,)),
                dma((3, chunks)), dma((2, chunks)), dma((2, chunks)), dma((3, chunks + 1)), dma((3, 2)),
            ],
            compiler_params=pltpu.CompilerParams(collective_id=0, has_side_effects=True, vmem_limit_bytes=67000000),
        )(x, dy, w_gate, w_up, w_down)
        shapes = [jax.ShapeDtypeStruct(w.shape, BF16) for w in (w_gate, w_up, w_down)]
        return tuple(pl.pallas_call(
            hand_over,
            out_shape=shapes,
            in_specs=[hbm] * 3,
            out_specs=[hbm] * 3,
            scratch_shapes=[vmem(a.shape, a.dtype) for a in shapes] + [dma((3,)), dma((3,))],
        )(*outs[:3]))

    return jax.shard_map(
        step,
        mesh=mesh,
        in_specs=(P("rep", None, None),) * 2 + (P("pp", None, None),) * 3,
        out_specs=(P(("rep", "pp"), None, None),) * 3,
        check_vma=False,
    )
```

```python
import functools

import jax
import jax.numpy as jnp
from jax import lax
from jax.experimental import pallas as pl
from jax.experimental.pallas import tpu as pltpu
from jax.sharding import PartitionSpec as P

F32, BF16 = jnp.float32, jnp.bfloat16
ROWS = 256
COLS = 256
EPS = 1e-6


LEAD = (1, 2, 5, 6, 9, 10, 14, 16)
LAG = (15, 14, 11, 10, 7, 6, 2, 2)


def at_stage(table, stages, me):
    number = 0
    for stage in range(stages):
        number = jnp.where(me == stage, table[min(stages - 1 - stage, len(table) - 1)], number)
    return number


def dot(a, b):
    return jnp.dot(a, b, preferred_element_type=F32)


def kernel(stages, x, dy, wg_in, wu_in, wd_in, og, ou, od, hp, hq, ha, hg, hu,
           wg, wu, wd, wgt, wut, wdt, acc_g, acc_u, acc_d, hs, ds, norm, turned, turned_dy,
           st_p, st_q, st_a, st_g, st_u, in_p, in_q, w_a, w_g, w_u, onward, back,
           sem_w, sem_h, sem_d, sem_f, sem_b, sem_st, sem_by, sem_in, sem_wt, sem_out):
    micro, tokens, d = x.shape
    ff = wg_in.shape[-1]
    chunks, tiles = tokens // ROWS, ff // COLS
    me = lax.axis_index("pp")
    first, last = me == 0, me == stages - 1
    inner = jnp.logical_not(last)
    later = jnp.logical_not(first)
    ahead, lag = at_stage(LEAD, stages, me), at_stage(LAG, stages, me)

    weights = [pltpu.make_async_copy(src.at[0], dst, sem_w.at[i]) for i, (src, dst) in enumerate(((wg_in, wg), (wu_in, wu), (wd_in, wd)))]

    def rows(c):
        return pl.ds(c * ROWS, ROWS)

    def load_x(i, c):
        return pltpu.make_async_copy(x.at[i, rows(c)], hs.at[i, rows(c)], sem_h.at[i, c])

    def load_dy(i, c):
        return pltpu.make_async_copy(dy.at[i, rows(c)], ds.at[i, rows(c)], sem_d.at[i, c])

    def send_h(i, c):
        slot = lax.rem(i, 2)
        return pltpu.make_async_remote_copy(onward.at[slot, c], hs.at[i, rows(c)], sem_f.at[slot, c], sem_h.at[i, c],
                                            device_id={"pp": me + 1}, device_id_type=pl.DeviceIdType.MESH)

    def send_d(i, c):
        return pltpu.make_async_remote_copy(back.at[c], ds.at[i, rows(c)], sem_b.at[c], sem_d.at[i, c],
                                            device_id={"pp": me - 1}, device_id_type=pl.DeviceIdType.MESH)

    def spill_act(i, c):
        return pltpu.make_async_copy(st_a.at[c], ha.at[i, rows(c)], sem_st.at[2, c])

    def spill(i, c):
        return [pltpu.make_async_copy(src.at[c], dst.at[i, rows(c)], sem_st.at[k, c]) for k, (src, dst) in enumerate(((st_p, hp), (st_q, hq)))]

    def spill_by(i, c):
        return [pltpu.make_async_copy(src.at[c], dst.at[i, rows(c)], sem_by.at[k, c]) for k, (src, dst) in enumerate(((st_g, hg), (st_u, hu)))]

    def fetch(i, c):
        return [pltpu.make_async_copy(src.at[i, rows(c)], dst.at[c], sem_in.at[k, c])
                for k, (src, dst) in enumerate(((hp, in_p), (hq, in_q)))]

    each = (tiles - chunks) // chunks
    groups = [range(chunks + c * each, chunks + (c + 1) * each) for c in range(chunks)] + [range(chunks)]

    def fetch_tiles(i, group):
        span = pl.ds(groups[group][0] * COLS, len(groups[group]) * COLS)
        return [pltpu.make_async_copy(src.at[i, :, span], dst.at[:, span], sem_wt.at[k, group])
                for k, (src, dst) in enumerate(((hg, w_g), (hu, w_u), (ha, w_a)))]

    @pl.when(first)
    def _():
        for c in range(chunks):
            load_x(0, c).start()

    for copy in weights:
        copy.start()

    @pl.when(first)
    def _():
        def body(i, _):
            for c in range(chunks):
                load_x(i, c).start()
            return 0
        lax.fori_loop(1, micro, body, 0)

    @pl.when(last)
    def _():
        def body(i, _):
            for c in range(chunks):
                load_dy(i, c).start()
            return 0
        lax.fori_loop(0, micro, body, 0)

    barrier = pltpu.get_barrier_semaphore()

    @pl.when(later)
    def _():
        pl.semaphore_signal(barrier, inc=1, device_id={"pp": me - 1}, device_id_type=pl.DeviceIdType.MESH)

    @pl.when(inner)
    def _():
        pl.semaphore_signal(barrier, inc=1, device_id={"pp": me + 1}, device_id_type=pl.DeviceIdType.MESH)

    for copy in weights:
        copy.wait()

    @pl.when(first | last)
    def _():
        pl.semaphore_wait(barrier, 1)

    @pl.when(later & inner)
    def _():
        pl.semaphore_wait(barrier, 2)

    def prepare():
        for n in range(tiles):
            cols = pl.ds(n * COLS, COLS)
            wgt[cols, :] = wg[:, cols].T
            wut[cols, :] = wu[:, cols].T
            wdt[:, cols] = wd[cols, :].T
            acc_g[:, cols] = jnp.zeros((d, COLS), F32)
            acc_u[:, cols] = jnp.zeros((d, COLS), F32)
            acc_d[:, cols] = jnp.zeros((d, COLS), F32)

    @pl.when(later)
    def _():
        prepare()

    def scale_of(wide):
        return lax.rsqrt(jnp.mean(wide * wide, -1, keepdims=True) + EPS)

    def term(i, n, left, right):
        return dot(left[lax.rem(i, 2)], right[:, pl.ds(n * COLS, COLS)]).astype(BF16).astype(F32)

    def weight(i, n, acc, left, right):
        acc[:, pl.ds(n * COLS, COLS)] += term(i, n, left, right)

    def turn(i, c):
        i = jnp.clip(i, 0, micro - 1)
        wide = hs[i, rows(c), :].astype(F32)
        turned[lax.rem(i, 2), :, rows(c)] = (wide * scale_of(wide)).astype(BF16).T
        turned_dy[lax.rem(i, 2), :, rows(c)] = ds[i, rows(c), :].T

    def parts(tile_numbers):
        return [(n, *arrays) for n in tile_numbers for arrays in ((acc_g, turned, w_g), (acc_u, turned, w_u), (acc_d, turned_dy, w_a))]

    def forward(i, c, onwards, w):
        fill = [] if w is None else parts([c])
        wide = hs[i, rows(c), :].astype(F32)
        norm[...] = (wide * scale_of(wide)).astype(BF16)
        for part in fill[:2]:
            weight(w, *part)
        for n in range(tiles):
            cols = pl.ds(n * COLS, COLS)
            gate = dot(norm[...], wg[:, cols])
            up = dot(norm[...], wu[:, cols])
            sig = 1.0 / (1.0 + jnp.exp(-gate))
            silu = gate * sig
            slope = up * (sig + silu * (1.0 - sig))
            act = (silu * up).astype(BF16)
            if onwards:
                st_p[c, :, cols] = silu
                st_q[c, :, cols] = slope
            else:
                in_p[c, :, cols] = silu
                in_q[c, :, cols] = slope
            st_a[c, :, cols] = act
        for part in fill[2:]:
            weight(w, *part)
        if onwards:
            out = dot(st_a[c], wd[...]).astype(BF16)
            onward[lax.rem(i, 2), c] = (hs[i, rows(c), :].astype(F32) + out.astype(F32)).astype(BF16)
            send_h(i, c).start()
            for copy in spill(i, c):
                copy.start()
        spill_act(i, c).start()

    def backward(i, c, w, upcoming):
        fill = [] if w is None else parts(groups[c])
        wide = hs[i, rows(c), :].astype(F32)
        scale = scale_of(wide)
        turn(upcoming, c)
        for n in range(tiles):
            cols = pl.ds(n * COLS, COLS)
            by_act = dot(ds[i, rows(c), :], wdt[:, cols]).astype(BF16).astype(F32)
            st_g[c, :, cols] = (by_act * in_q[c, :, cols]).astype(BF16)
            st_u[c, :, cols] = (by_act * in_p[c, :, cols]).astype(BF16)
        for part in fill[:2]:
            weight(w, *part)
        by_gate = dot(st_g[c], wgt[...]).astype(BF16)
        by_up = dot(st_u[c], wut[...]).astype(BF16)
        by_a = (by_gate.astype(F32) + by_up.astype(F32)).astype(BF16).astype(F32)
        along = jnp.mean(by_a * wide, -1, keepdims=True) * (scale * scale * scale)
        by_h = (by_a * scale - wide * along).astype(BF16)
        back[c] = (ds[i, rows(c), :].astype(F32) + by_h.astype(F32)).astype(BF16)
        for part in fill[2:]:
            weight(w, *part)

    def step(t, _):
        b = t - ahead
        w = b - lag
        has_f, has_b, has_w = t < micro, (b >= 0) & (b < micro), w >= 0
        final = b == micro - 1
        fetches = inner & (b >= -1) & (b < micro - 1)
        next_w = w >= -1

        def refill(group):
            @pl.when(next_w)
            def _():
                for copy in fetch_tiles(w + 1, group):
                    copy.start()

        def ready(some):
            @pl.when(has_w)
            def _():
                for group in some:
                    for copy in fetch_tiles(w, group):
                        copy.wait()

        @pl.when((b > 0) & (b <= micro))
        def _():
            for c in range(chunks):
                for copy in spill_by(b - 1, c):
                    copy.wait()

        for c in range(chunks):
            ready([c])

            @pl.when(has_b)
            def _():
                @pl.when(last)
                def _():
                    load_dy(b, c).wait()

                @pl.when(later & (b > 0))
                def _():
                    send_d(b - 1, c).wait_send()

                @pl.when(inner)
                def _():
                    for copy in fetch(b, c):
                        copy.wait()
                    send_d(b, c).wait_recv()

            @pl.when(has_b & has_w & jnp.logical_not(final))
            def _():
                backward(b, c, w, w + 1)

            @pl.when(has_b & (jnp.logical_not(has_w) | final))
            def _():
                backward(b, c, None, w + 1)

            @pl.when(has_w & jnp.logical_not(has_b))
            def _():
                turn(w + 1, c)
                for part in parts(groups[c]):
                    weight(w, *part)

            @pl.when(has_b & later)
            def _():
                send_d(b, c).start()

            @pl.when(has_b)
            def _():
                for copy in spill_by(b, c):
                    copy.start()

            @pl.when((t > 0) & (t <= micro))
            def _():
                spill_act(t - 1, c).wait()

            @pl.when(inner & (t > 0) & (t <= micro))
            def _():
                for copy in spill(t - 1, c):
                    copy.wait()

            @pl.when(fetches)
            def _():
                for copy in fetch(b + 1, c):
                    copy.start()

            @pl.when(jnp.logical_not(final))
            def _():
                refill(c)

        @pl.when(has_w & final)
        def _():
            for part in parts(range(chunks, tiles)):
                weight(w, *part)

        @pl.when(final)
        def _():
            for c in range(chunks):
                refill(c)

        ready([chunks])

        for c in range(chunks):
            @pl.when(has_f)
            def _():
                @pl.when(first)
                def _():
                    load_x(t, c).wait()

                @pl.when(later)
                def _():
                    send_h(t, c).wait_recv()

                @pl.when(inner & (t > 1))
                def _():
                    send_h(t - 2, c).wait_send()

            for onwards in (True, False):
                at = inner if onwards else last

                @pl.when(has_f & at & has_w)
                def _():
                    forward(t, c, onwards, w)

                @pl.when(has_f & at & jnp.logical_not(has_w))
                def _():
                    forward(t, c, onwards, None)

        @pl.when(first & (t == 0))
        def _():
            prepare()

        @pl.when(has_w & jnp.logical_not(has_f))
        def _():
            for part in parts(range(chunks)):
                weight(w, *part)

        refill(chunks)
        return 0

    lax.fori_loop(0, micro + ahead + lag - 1, step, 0)

    end = micro - 1

    for group in range(chunks + 1):
        for copy in fetch_tiles(end, group):
            copy.wait()
    results = []
    for part in range(2):
        some = range(part * tiles // 2, (part + 1) * tiles // 2)
        for n in some:
            cols = pl.ds(n * COLS, COLS)
            wg[:, cols] = (acc_g[:, cols] + term(end, n, turned, w_g)).astype(BF16)
            wu[:, cols] = (acc_u[:, cols] + term(end, n, turned, w_u)).astype(BF16)
            wd[cols, :] = (acc_d[:, cols] + term(end, n, turned_dy, w_a)).astype(BF16).T
        span = pl.ds(some[0] * COLS, len(some) * COLS)
        copies = [pltpu.make_async_copy(wg.at[:, span], og.at[0, :, span], sem_out.at[0, part]),
                  pltpu.make_async_copy(wu.at[:, span], ou.at[0, :, span], sem_out.at[1, part]),
                  pltpu.make_async_copy(wd.at[span], od.at[0, span], sem_out.at[2, part])]
        for copy in copies:
            copy.start()
        results += copies

    @pl.when(later)
    def _():
        for c in range(chunks):
            send_d(end, c).wait_send()

    @pl.when(inner)
    def _():
        for c in range(chunks):
            send_h(micro - 2, c).wait_send()
            send_h(micro - 1, c).wait_send()

    for copy in results:
        copy.wait()


def hand_over(*refs):
    sources, results, held, sem_in, sem_out = refs[:3], refs[3:6], refs[6:9], refs[9], refs[10]
    reads = [pltpu.make_async_copy(a, b, sem_in.at[i]) for i, (a, b) in enumerate(zip(sources, held, strict=True))]
    writes = [pltpu.make_async_copy(a, b, sem_out.at[i]) for i, (a, b) in enumerate(zip(held, results, strict=True))]
    for copy in reads:
        copy.start()
    for read, write in zip(reads, writes, strict=True):
        read.wait()
        write.start()
    for copy in writes:
        copy.wait()


def solution(mesh):
    stages = mesh.shape["pp"]

    def step(x, dy, w_gate, w_up, w_down):
        micro, tokens, d = x.shape
        ff = w_gate.shape[-1]
        chunks = tokens // ROWS
        hbm = pl.BlockSpec(memory_space=pl.ANY)
        vmem, dma = pltpu.VMEM, pltpu.SemaphoreType.DMA
        outs = pl.pallas_call(
            functools.partial(kernel, stages),
            out_shape=[
                jax.ShapeDtypeStruct(w_gate.shape, BF16),
                jax.ShapeDtypeStruct(w_up.shape, BF16),
                jax.ShapeDtypeStruct(w_down.shape, BF16),
                jax.ShapeDtypeStruct((micro, tokens, ff), F32),
                jax.ShapeDtypeStruct((micro, tokens, ff), F32),
                jax.ShapeDtypeStruct((micro, tokens, ff), BF16),
                jax.ShapeDtypeStruct((micro, tokens, ff), BF16),
                jax.ShapeDtypeStruct((micro, tokens, ff), BF16),
            ],
            in_specs=[hbm] * 5,
            out_specs=[hbm] * 8,
            scratch_shapes=[
                vmem((d, ff), BF16), vmem((d, ff), BF16), vmem((ff, d), BF16),
                vmem((ff, d), BF16), vmem((ff, d), BF16), vmem((d, ff), BF16),
                vmem((d, ff), F32), vmem((d, ff), F32), vmem((d, ff), F32),
                vmem((micro, tokens, d), BF16), vmem((micro, tokens, d), BF16),
                vmem((ROWS, d), BF16), vmem((2, d, tokens), BF16), vmem((2, d, tokens), BF16),
                vmem((chunks, ROWS, ff), F32), vmem((chunks, ROWS, ff), F32),
                vmem((chunks, ROWS, ff), BF16), vmem((chunks, ROWS, ff), BF16), vmem((chunks, ROWS, ff), BF16),
                vmem((chunks, ROWS, ff), F32), vmem((chunks, ROWS, ff), F32),
                vmem((tokens, ff), BF16), vmem((tokens, ff), BF16), vmem((tokens, ff), BF16),
                vmem((2, chunks, ROWS, d), BF16), vmem((chunks, ROWS, d), BF16),
                dma((3,)), dma((micro, chunks)), dma((micro, chunks)), dma((2, chunks)), dma((chunks,)),
                dma((3, chunks)), dma((2, chunks)), dma((2, chunks)), dma((3, chunks + 1)), dma((3, 2)),
            ],
            compiler_params=pltpu.CompilerParams(collective_id=0, has_side_effects=True, vmem_limit_bytes=67000000),
        )(x, dy, w_gate, w_up, w_down)
        shapes = [jax.ShapeDtypeStruct(w.shape, BF16) for w in (w_gate, w_up, w_down)]
        return tuple(pl.pallas_call(
            hand_over,
            out_shape=shapes,
            in_specs=[hbm] * 3,
            out_specs=[hbm] * 3,
            scratch_shapes=[vmem(a.shape, a.dtype) for a in shapes] + [dma((3,)), dma((3,))],
        )(*outs[:3]))

    return jax.shard_map(
        step,
        mesh=mesh,
        in_specs=(P("rep", None, None),) * 2 + (P("pp", None, None),) * 3,
        out_specs=(P(("rep", "pp"), None, None),) * 3,
        check_vma=False,
    )
```
